128 devices in a mesh: pod: 1, dp: 16 (over z, y), sp: 8 (over x, core).
Axes of the slice: x: 4, y: 4, z: 4, core: 2. Of those that a mesh axis runs over, the one named last changes fastest.
Arguments:
- x: bfloat16 [48, 24, 128, 1152], P(('pod', 'dp'), 'sp')
- norm_gain: bfloat16 [2, 2, 1152], replicated
- norm_shift: bfloat16 [2, 2, 1152], replicated
- w_qkv: bfloat16 [2, 3, 1152, 16, 72], replicated
- w_out: bfloat16 [2, 16, 72, 1152], replicated
- w_up: bfloat16 [2, 1152, 4608], replicated
- w_down: bfloat16 [2, 4608, 1152], replicated
Outputs:
- output: bfloat16 [48, 24, 128, 1152], P(('pod', 'dp'), 'sp')
All inputs are finite; a program needn't handle non-finite values.
Results may differ from the reference program's by a relative error of at most 0.0161672.
Values are sent between devices in bfloat16 or wider.
A program may use at most 1 GiB of HBM per device.

```python
import jax
import jax.numpy as jnp
from jax import lax

NUM_VIDEOS = 48
NUM_FRAMES = 24
NUM_PATCHES = 128
MODEL_WIDTH = 1152
NUM_HEADS = 16

HEAD_DIM = MODEL_WIDTH // NUM_HEADS
FF_WIDTH = 4 * MODEL_WIDTH
LN_EPS = 1e-6
QK_GAIN = 1.5


def layer_norm(tokens, gain, shift):
    tok_f = tokens.astype(jnp.float32)
    mean_val = jnp.mean(tok_f, axis=-1, keepdims=True)
    centered = tok_f - mean_val
    var_val = jnp.mean(centered * centered, axis=-1, keepdims=True)
    normed = centered * lax.rsqrt(var_val + LN_EPS)
    return (normed * gain.astype(jnp.float32) + shift.astype(jnp.float32)).astype(jnp.bfloat16)


def seq_block(tokens, gains, shifts, w_qkv, w_out, w_up, w_down):
    normed = layer_norm(tokens, gains[0], shifts[0])
    proj_qkv = jnp.einsum('ld,kdhe->klhe', normed.astype(jnp.float32), w_qkv.astype(jnp.float32)).astype(jnp.bfloat16)
    scores = jnp.einsum('lhe,mhe->hlm', proj_qkv[0].astype(jnp.float32), proj_qkv[1].astype(jnp.float32)) * (HEAD_DIM ** -0.5)
    attn_probs = jax.nn.softmax(scores, axis=-1).astype(jnp.bfloat16)
    mixed = jnp.einsum('hlm,mhe->lhe', attn_probs.astype(jnp.float32), proj_qkv[2].astype(jnp.float32)).astype(jnp.bfloat16)
    attn_proj = jnp.einsum('lhe,hed->ld', mixed.astype(jnp.float32), w_out.astype(jnp.float32)).astype(jnp.bfloat16)
    hidden = (tokens.astype(jnp.float32) + attn_proj.astype(jnp.float32)).astype(jnp.bfloat16)
    normed_mlp = layer_norm(hidden, gains[1], shifts[1])
    up_proj = jnp.dot(normed_mlp, w_up, preferred_element_type=jnp.float32).astype(jnp.bfloat16)
    activated = jax.nn.gelu(up_proj.astype(jnp.float32), approximate=True).astype(jnp.bfloat16)
    down_proj = jnp.dot(activated, w_down, preferred_element_type=jnp.float32).astype(jnp.bfloat16)
    return (hidden.astype(jnp.float32) + down_proj.astype(jnp.float32)).astype(jnp.bfloat16)


def setup_inputs(seed: int = 0, part: int = 0) -> dict:
    base_key = jax.random.key(seed)
    key_list = jax.random.split(base_key, 7)
    data_key = jax.random.fold_in(key_list[0], part)
    key_frame, key_patch, key_noise = jax.random.split(data_key, 3)
    frame_code = jax.random.normal(key_frame, (NUM_VIDEOS, NUM_FRAMES, 1, MODEL_WIDTH), jnp.float32)
    patch_code = jax.random.normal(key_patch, (NUM_VIDEOS, 1, NUM_PATCHES, MODEL_WIDTH), jnp.float32)
    noise_val = jax.random.normal(key_noise, (NUM_VIDEOS, NUM_FRAMES, NUM_PATCHES, MODEL_WIDTH), jnp.float32)
    x = (frame_code + patch_code + 0.5 * noise_val).astype(jnp.bfloat16)
    norm_gain = (1.0 + 0.4 * jax.random.normal(key_list[1], (2, 2, MODEL_WIDTH), jnp.float32)).astype(jnp.bfloat16)
    norm_shift = (0.4 * jax.random.normal(key_list[2], (2, 2, MODEL_WIDTH), jnp.float32)).astype(jnp.bfloat16)
    qkv_gain = jnp.array([QK_GAIN, QK_GAIN, 1.0], jnp.float32).reshape(1, 3, 1, 1, 1)
    w_qkv = (jax.random.normal(key_list[3], (2, 3, MODEL_WIDTH, NUM_HEADS, HEAD_DIM), jnp.float32) * (MODEL_WIDTH ** -0.5) * qkv_gain).astype(jnp.bfloat16)
    w_out = (jax.random.normal(key_list[4], (2, NUM_HEADS, HEAD_DIM, MODEL_WIDTH), jnp.float32) * (MODEL_WIDTH ** -0.5)).astype(jnp.bfloat16)
    w_up = (jax.random.normal(key_list[5], (2, MODEL_WIDTH, FF_WIDTH), jnp.float32) * (MODEL_WIDTH ** -0.5)).astype(jnp.bfloat16)
    w_down = (jax.random.normal(key_list[6], (2, FF_WIDTH, MODEL_WIDTH), jnp.float32) * (FF_WIDTH ** -0.5)).astype(jnp.bfloat16)
    return {'x': x, 'norm_gain': norm_gain, 'norm_shift': norm_shift, 'w_qkv': w_qkv, 'w_out': w_out, 'w_up': w_up, 'w_down': w_down}


def reference(x, norm_gain, norm_shift, w_qkv, w_out, w_up, w_down):
    num_videos, num_frames, num_patches, model_width = x.shape

    def spatial_fn(frame_tok):
        return seq_block(frame_tok, norm_gain[0], norm_shift[0], w_qkv[0], w_out[0], w_up[0], w_down[0])

    def temporal_fn(tube_tok):
        return seq_block(tube_tok, norm_gain[1], norm_shift[1], w_qkv[1], w_out[1], w_up[1], w_down[1])

    frame_rows = x.reshape(num_videos * num_frames, num_patches, model_width)
    spatial_out = lax.map(spatial_fn, frame_rows).reshape(num_videos, num_frames, num_patches, model_width)
    tube_rows = jnp.transpose(spatial_out, (0, 2, 1, 3)).reshape(num_videos * num_patches, num_frames, model_width)
    temporal_out = lax.map(temporal_fn, tube_rows).reshape(num_videos, num_patches, num_frames, model_width)
    return jnp.transpose(temporal_out, (0, 2, 1, 3))
```

```python
import functools

import jax
import jax.numpy as jnp
from jax import lax
from jax.experimental import pallas as pl
from jax.experimental.pallas import tpu as pltpu
from jax.sharding import PartitionSpec as P

LN_EPS = 1e-6
F32, BF16 = jnp.float32, jnp.bfloat16
UP_COLS = 512
LN_ROWS = 32
TANH_IN = 0.7978845608028654
TANH_CUBE = 0.044715


def gelu(u):
    inner = u * (TANH_IN + (TANH_IN * TANH_CUBE) * (u * u))
    half = 0.5 * u
    return half + half * jnp.tanh(inner)


def dot_nt(a, b):
    return lax.dot_general(a, b, (((1,), (1,)), ((), ())), preferred_element_type=F32)


def dot_nn(a, b):
    return jnp.dot(a, b, preferred_element_type=F32)


def ln_rows(tok, gain, shift):
    mean = jnp.mean(tok, axis=-1, keepdims=True)
    cen = tok - mean
    var = jnp.mean(cen * cen, axis=-1, keepdims=True)
    return (cen * lax.rsqrt(var + LN_EPS) * gain + shift).astype(BF16)


def kernel(dims, x_hbm, gain_ref, shift_ref, wqkv_hbm, wout_hbm, wup_hbm, wdown_hbm, y_hbm,
           xs, ns, rx, osend, orecv, wq, wo, wu, wd, nbuf, qkv, obuf, ubuf, gbuf, of32,
           xsem, wsem, ysem, send1, recv1, send2, recv2):
    nv, fr, npat, width, heads, hd, ff, n = dims
    rows = fr * npat
    pp = npat // n
    frames = fr * n
    me = lax.axis_index('sp')
    scale = hd ** -0.5
    barrier = pltpu.get_barrier_semaphore()

    def w_copy(block, which):
        if which < 3:
            return pltpu.make_async_copy(wqkv_hbm.at[block, which], wq.at[which], wsem.at[which])
        src, dst = [(wout_hbm, wo), (wup_hbm, wu), (wdown_hbm, wd)][which - 3]
        return pltpu.make_async_copy(src.at[block], dst, wsem.at[which])

    def x_copy(v):
        return pltpu.make_async_copy(x_hbm.at[v], xs.at[v], xsem.at[v])

    x_copy(0).start()
    for which in range(6):
        w_copy(0, which).start()
    for v in range(1, nv):
        x_copy(v).start()

    for step in range(1, n):
        peer = lax.rem(me + step, n)
        pl.semaphore_signal(barrier, inc=1, device_id={'sp': peer}, device_id_type=pl.DeviceIdType.MESH)

    def norm(v, block, which, write):
        gain = gain_ref[block, which:which + 1, :].astype(F32)
        shift = shift_ref[block, which:which + 1, :].astype(F32)
        for f in range(fr):
            for r in range(0, npat, LN_ROWS):
                write(f, r, ln_rows(xs[v, f, r:r + LN_ROWS, :].astype(F32), gain, shift))

    def to_nbuf(f, r, val):
        nbuf[f * npat + r:f * npat + r + LN_ROWS, :] = val

    def head_attn(qs, ks, vs, keep, write):
        tiles = width // 128
        lane = lax.broadcasted_iota(jnp.int32, (1, 128), 1)
        outs = [None] * tiles
        for h in range(heads):
            lo, hi = h * hd, (h + 1) * hd
            t0, t1 = lo // 128, (hi - 1) // 128
            q_parts = []
            for t in range(t0, t1 + 1):
                inside = (lane + t * 128 >= lo) & (lane + t * 128 < hi)
                part = qs(t)
                q_parts.append(jnp.where(inside, part, jnp.zeros_like(part)))
            qw = q_parts[0] if t0 == t1 else jnp.concatenate(q_parts, axis=1)
            s = dot_nt(qw, ks(t0, t1 + 1))
            s = keep(s)
            m = jnp.max(s, axis=-1, keepdims=True)
            e = jnp.exp((s - m) * scale)
            p = (e * (1.0 / jnp.sum(e, axis=-1, keepdims=True))).astype(BF16)
            o = dot_nn(p, vs(t0, t1 + 1))
            for t in range(t0, t1 + 1):
                part = o[:, (t - t0) * 128:(t - t0 + 1) * 128]
                if outs[t] is None:
                    outs[t] = part
                else:
                    outs[t] = jnp.where(lane + t * 128 >= lo, part, outs[t])
            for t in range(t0, t1 + 1):
                if (t + 1) * 128 <= hi:
                    write(t, outs[t])
                    outs[t] = None

    def tail(v, block, attn, first):
        @pl.when(first)
        def _():
            w_copy(block, 3).wait()
        a = dot_nn(attn, wo[...]).astype(BF16)
        for f in range(fr):
            h = xs[v, f].astype(F32) + a[f * npat:(f + 1) * npat].astype(F32)
            xs[v, f] = h.astype(BF16)
        norm(v, block, 1, to_nbuf)

        @pl.when(first)
        def _():
            w_copy(block, 4).wait()

        def up(c):
            cols = pl.ds(pl.multiple_of(c * UP_COLS, UP_COLS), UP_COLS)
            return dot_nn(nbuf[...], wu[:, cols]).astype(BF16)

        def act(c):
            cols = pl.ds(pl.multiple_of(c * UP_COLS, UP_COLS), UP_COLS)
            gbuf[:, cols] = gelu(ubuf[...].astype(F32)).astype(BF16)

        ubuf[...] = up(0)

        def up_step(c, carry):
            act(c - 1)
            ubuf[...] = up(c)
            return carry

        lax.fori_loop(1, ff // UP_COLS, up_step, 0)
        act(ff // UP_COLS - 1)

        @pl.when(first)
        def _():
            w_copy(block, 5).wait()

        def down(lo, cols):
            part = dot_nn(gbuf[...], wd[:, lo:lo + cols]).astype(BF16)
            for f in range(fr):
                h = xs[v, f, :, lo:lo + cols].astype(F32) + part[f * npat:(f + 1) * npat].astype(F32)
                xs[v, f, :, lo:lo + cols] = h.astype(BF16)

        for lo in range(0, width, 512):
            down(lo, min(512, width - lo))

    def send_copy(v, peer, stage):
        if stage == 1:
            return pltpu.make_async_remote_copy(
                src_ref=ns.at[v, :, pl.ds(pl.multiple_of(peer * pp, pp), pp), :],
                dst_ref=rx.at[v, pl.ds(me * fr, fr)],
                send_sem=send1.at[v, peer], recv_sem=recv1.at[v, me],
                device_id={'sp': peer}, device_id_type=pl.DeviceIdType.MESH)
        return pltpu.make_async_remote_copy(
            src_ref=osend.at[v, pl.ds(peer * fr, fr)],
            dst_ref=orecv.at[v, :, pl.ds(pl.multiple_of(me * pp, pp), pp), :],
            send_sem=send2.at[v, peer], recv_sem=recv2.at[v, me],
            device_id={'sp': peer}, device_id_type=pl.DeviceIdType.MESH)

    def recv_wait(v, peer, stage):
        if stage == 1:
            dst = rx.at[v, pl.ds(peer * fr, fr)]
            sem = recv1.at[v, peer]
        else:
            dst = orecv.at[v, :, pl.ds(pl.multiple_of(peer * pp, pp), pp), :]
            sem = recv2.at[v, peer]
        pltpu.make_async_copy(dst, dst, sem).wait()

    def each_peer(fn):
        for step in range(1, n):
            fn(lax.rem(me + step, n))

    def spatial(v, carry):
        x_copy(v).wait()
        norm(v, 0, 0, to_nbuf)

        def project(j, c):
            @pl.when(v == 0)
            def _():
                pltpu.make_async_copy(wqkv_hbm.at[0, j], wq.at[j], wsem.at[j]).wait()
            qkv[j] = dot_nt(nbuf[...], wq[j]).astype(BF16)
            return c

        lax.fori_loop(0, 3, project, 0)

        @pl.when(v == nv - 1)
        def _():
            for which in range(3):
                w_copy(1, which).start()

        def frame(f, c):
            rs = pl.ds(pl.multiple_of(f * npat, npat), npat)

            def write(t, val):
                obuf[rs, t * 128:(t + 1) * 128] = val.astype(BF16)

            head_attn(lambda t: qkv[0, rs, t * 128:(t + 1) * 128],
                      lambda a, b: qkv[1, rs, a * 128:b * 128],
                      lambda a, b: qkv[2, rs, a * 128:b * 128],
                      lambda s: s, write)
            return c

        lax.fori_loop(0, fr, frame, 0)
        tail(v, 0, obuf[...], v == 0)

        @pl.when(v == nv - 1)
        def _():
            for which in range(3, 6):
                w_copy(1, which).start()

        def to_ns(f, r, val):
            ns[v, f, r:r + LN_ROWS, :] = val

        norm(v, 1, 0, to_ns)

        @pl.when(v == 0)
        def _():
            pl.semaphore_wait(barrier, n - 1)

        rx[v, pl.ds(me * fr, fr)] = ns[v, :, pl.ds(pl.multiple_of(me * pp, pp), pp), :]
        each_peer(lambda peer: send_copy(v, peer, 1).start())
        return carry

    lax.fori_loop(0, nv, spatial, 0)

    half = 8
    groups = pp // half
    grows = frames * half

    def temporal(v, carry):
        each_peer(lambda peer: recv_wait(v, peer, 1))
        tok = rx[v].reshape(rows, width)

        def project(j, c):
            @pl.when(v == 0)
            def _():
                pltpu.make_async_copy(wqkv_hbm.at[1, j], wq.at[j], wsem.at[j]).wait()
            val = dot_nt(rx[v].reshape(rows, width), wq[j]).reshape(frames, groups, half, width)
            for g in range(groups):
                qkv[j, g * grows:(g + 1) * grows, :] = val[:, g].reshape(grows, width).astype(BF16)
            return c

        lax.fori_loop(0, 3, project, 0)
        sub = lax.broadcasted_iota(jnp.int32, (1, half, grows), 1)
        key = lax.broadcasted_iota(jnp.int32, (1, half, grows), 2)
        same = sub == lax.rem(key, half)

        def keep(s):
            return jnp.where(same, s.reshape(frames, half, grows), -jnp.inf).reshape(grows, grows)

        def group(g, c):
            rs = pl.ds(pl.multiple_of(g * grows, grows), grows)

            def write(t, val):
                of32[:, g, :, t * 128:(t + 1) * 128] = val.reshape(frames, half, 128)

            head_attn(lambda t: qkv[0, rs, t * 128:(t + 1) * 128],
                      lambda a, b: qkv[1, rs, a * 128:b * 128],
                      lambda a, b: qkv[2, rs, a * 128:b * 128],
                      keep, write)
            return c

        lax.fori_loop(0, groups, group, 0)
        for f in range(frames):
            osend[v, f] = of32[f].reshape(pp, width).astype(BF16)
        orecv[v, :, pl.ds(pl.multiple_of(me * pp, pp), pp), :] = osend[v, pl.ds(me * fr, fr)]
        each_peer(lambda peer: send_copy(v, peer, 2).start())
        return carry

    lax.fori_loop(0, nv, temporal, 0)

    def y_copy(v):
        return pltpu.make_async_copy(xs.at[v], y_hbm.at[v], ysem.at[v])

    def finish(v, carry):
        each_peer(lambda peer: recv_wait(v, peer, 2))
        tail(v, 1, orecv[v].reshape(rows, width), v == 0)
        y_copy(v).start()
        return carry

    lax.fori_loop(0, nv, finish, 0)
    for v in range(nv):
        y_copy(v).wait()
        each_peer(lambda peer: send_copy(v, peer, 1).wait_send())
        each_peer(lambda peer: send_copy(v, peer, 2).wait_send())


def solution(mesh):
    tok_spec = P(('pod', 'dp'), 'sp', None, None)
    n = mesh.shape['sp']

    def local_step(x, gain, shift, w_qkv, w_out, w_up, w_down):
        nv, fr, npat, width = x.shape
        heads, hd = w_qkv.shape[3:]
        ff = w_up.shape[2]
        rows = fr * npat
        wqkv_t = jnp.transpose(w_qkv, (0, 1, 3, 4, 2)).reshape(2, 3, heads * hd, width)
        wout_r = w_out.reshape(2, heads * hd, width)
        dims = (nv, fr, npat, width, heads, hd, ff, n)
        hbm = pl.BlockSpec(memory_space=pl.ANY)
        vmem = pl.BlockSpec(memory_space=pltpu.VMEM)
        pp, frames = npat // n, fr * n
        return pl.pallas_call(
            functools.partial(kernel, dims),
            out_shape=jax.ShapeDtypeStruct(x.shape, BF16),
            in_specs=[hbm, vmem, vmem, hbm, hbm, hbm, hbm],
            out_specs=hbm,
            scratch_shapes=[
                pltpu.VMEM((nv, fr, npat, width), BF16),
                pltpu.VMEM((nv, fr, npat, width), BF16),
                pltpu.VMEM((nv, frames, pp, width), BF16),
                pltpu.VMEM((nv, frames, pp, width), BF16),
                pltpu.VMEM((nv, fr, npat, width), BF16),
                pltpu.VMEM((3, heads * hd, width), BF16),
                pltpu.VMEM((heads * hd, width), BF16),
                pltpu.VMEM((width, ff), BF16),
                pltpu.VMEM((ff, width), BF16),
                pltpu.VMEM((rows, width), BF16),
                pltpu.VMEM((3, rows, heads * hd), BF16),
                pltpu.VMEM((rows, heads * hd), BF16),
                pltpu.VMEM((rows, UP_COLS), BF16),
                pltpu.VMEM((rows, ff), BF16),
                pltpu.VMEM((frames, pp // 8, 8, width), F32),
                pltpu.SemaphoreType.DMA((nv,)),
                pltpu.SemaphoreType.DMA((6,)),
                pltpu.SemaphoreType.DMA((nv,)),
                pltpu.SemaphoreType.DMA((nv, n)),
                pltpu.SemaphoreType.DMA((nv, n)),
                pltpu.SemaphoreType.DMA((nv, n)),
                pltpu.SemaphoreType.DMA((nv, n)),
            ],
            compiler_params=pltpu.CompilerParams(
                collective_id=0, has_side_effects=True, vmem_limit_bytes=67_000_000),
        )(x, gain, shift, wqkv_t, wout_r, w_up, w_down)

    return jax.shard_map(local_step, mesh=mesh, in_specs=(tok_spec, P(), P(), P(), P(), P(), P()), out_specs=tok_spec, check_vma=False)
```

```python
import functools

import jax
import jax.numpy as jnp
from jax import lax
from jax.experimental import pallas as pl
from jax.experimental.pallas import tpu as pltpu
from jax.sharding import PartitionSpec as P

LN_EPS = 1e-6
F32, BF16 = jnp.float32, jnp.bfloat16
UP_COLS = 512
LN_ROWS = 32
ATT_BUFS = 6
QKV_SPLIT = 1792
TANH_IN = 0.7978845608028654
TANH_CUBE = 0.044715


def gelu(u):
    inner = u * (TANH_IN + (TANH_IN * TANH_CUBE) * (u * u))
    half = 0.5 * u
    return half + half * jnp.tanh(inner)


def dot_nt(a, b):
    return lax.dot_general(a, b, (((1,), (1,)), ((), ())), preferred_element_type=F32)


def dot_nn(a, b):
    return jnp.dot(a, b, preferred_element_type=F32)


def ln_rows(tok, gain, shift):
    mean = jnp.mean(tok, axis=-1, keepdims=True)
    cen = tok - mean
    var = jnp.mean(cen * cen, axis=-1, keepdims=True)
    return (cen * lax.rsqrt(var + LN_EPS) * gain + shift).astype(BF16)


def kernel(dims, x_hbm, gain_ref, shift_ref, wqkv_hbm, wout_hbm, wup_hbm, wdown_hbm, y_hbm,
           xs, ns, rx, osend, orecv, wq, wo, wu, wd, nbuf, qkv, obuf, ubuf, gbuf, of32, sbuf, pbuf,
           xsem, wsem, ysem, send1, recv1, send2, recv2):
    nv, fr, npat, width, heads, hd, ff, n = dims
    rows = fr * npat
    pp = npat // n
    frames = fr * n
    me = lax.axis_index('sp')
    scale = hd ** -0.5
    barrier = pltpu.get_barrier_semaphore()

    def w_copy(block, which):
        if which < 3:
            return pltpu.make_async_copy(wqkv_hbm.at[block, which], wq.at[which * width:(which + 1) * width], wsem.at[which])
        src, dst = [(wout_hbm, wo), (wup_hbm, wu), (wdown_hbm, wd)][which - 3]
        return pltpu.make_async_copy(src.at[block], dst, wsem.at[which])

    def x_copy(v):
        return pltpu.make_async_copy(x_hbm.at[v], xs.at[v], xsem.at[v])

    x_copy(0).start()
    for which in range(6):
        w_copy(0, which).start()
    for v in range(1, nv):
        x_copy(v).start()

    for step in range(1, n):
        peer = lax.rem(me + step, n)
        pl.semaphore_signal(barrier, inc=1, device_id={'sp': peer}, device_id_type=pl.DeviceIdType.MESH)

    def norm(v, block, which, write):
        gain = gain_ref[block, which:which + 1, :].astype(F32)
        shift = shift_ref[block, which:which + 1, :].astype(F32)
        for f in range(fr):
            for r in range(0, npat, LN_ROWS):
                write(f, r, ln_rows(xs[v, f, r:r + LN_ROWS, :].astype(F32), gain, shift))

    def to_nbuf(f, r, val):
        nbuf[f * npat + r:f * npat + r + LN_ROWS, :] = val

    def attend(units, masked):
        tiles = width // 128
        lane = lax.broadcasted_iota(jnp.int32, (1, 128), 1)
        outs = {}
        tops, sums = {}, {}

        def span(h):
            return h * hd, (h + 1) * hd, h * hd // 128, ((h + 1) * hd - 1) // 128 + 1

        def buf(i):
            return i % ATT_BUFS

        def score(i):
            base, nrow, h = units[i][:3]
            lo, hi, t0, t1 = span(h)
            parts = []
            for t in range(t0, t1):
                part = qkv[base:base + nrow, t * 128:(t + 1) * 128]
                inside = (lane + t * 128 >= lo) & (lane + t * 128 < hi)
                parts.append(jnp.where(inside, part, jnp.zeros_like(part)))
            qw = parts[0] if len(parts) == 1 else jnp.concatenate(parts, axis=1)
            keys = qkv[base:base + nrow, width + t0 * 128:width + t1 * 128]
            sbuf[buf(i), :nrow, :nrow] = masked(dot_nt(qw, keys))

        def top(i):
            nrow = units[i][1]
            tops[i] = jnp.max(sbuf[buf(i), :nrow, :nrow], axis=-1, keepdims=True)

        def expo(i):
            nrow = units[i][1]
            e = jnp.exp((sbuf[buf(i), :nrow, :nrow] - tops.pop(i)) * scale)
            sbuf[buf(i), :nrow, :nrow] = e
            sums[i] = jnp.sum(e, axis=-1, keepdims=True)

        def prob(i):
            nrow = units[i][1]
            pbuf[buf(i), :nrow, :nrow] = (sbuf[buf(i), :nrow, :nrow] * (1.0 / sums.pop(i))).astype(BF16)

        def mix(i):
            base, nrow, h, write = units[i]
            lo, hi, t0, t1 = span(h)
            o = dot_nn(pbuf[buf(i), :nrow, :nrow], qkv[base:base + nrow, 2 * width + t0 * 128:2 * width + t1 * 128])
            for t in range(t0, t1):
                part = o[:, (t - t0) * 128:(t - t0 + 1) * 128]
                if (base, t) in outs:
                    part = jnp.where(lane + t * 128 >= lo, part, outs.pop((base, t)))
                if (t + 1) * 128 <= hi:
                    write(t, part)
                else:
                    outs[(base, t)] = part

        stages = ((score, 0), (top, 2), (expo, 3), (prob, 4), (mix, 5))
        for i in range(len(units) + 5):
            for fn, lag in reversed(stages):
                if 0 <= i - lag < len(units):
                    fn(i - lag)

    def tail(v, block, attn, first):
        @pl.when(first)
        def _():
            w_copy(block, 3).wait()
        a = dot_nn(attn, wo[...]).astype(BF16)
        for f in range(fr):
            h = xs[v, f].astype(F32) + a[f * npat:(f + 1) * npat].astype(F32)
            xs[v, f] = h.astype(BF16)
        norm(v, block, 1, to_nbuf)

        @pl.when(first)
        def _():
            w_copy(block, 4).wait()

        def up(c):
            cols = pl.ds(pl.multiple_of(c * UP_COLS, UP_COLS), UP_COLS)
            return dot_nn(nbuf[...], wu[:, cols]).astype(BF16)

        def act(c):
            cols = pl.ds(pl.multiple_of(c * UP_COLS, UP_COLS), UP_COLS)
            gbuf[:, cols] = gelu(ubuf[...].astype(F32)).astype(BF16)

        ubuf[...] = up(0)

        def up_step(c, carry):
            act(c - 1)
            ubuf[...] = up(c)
            return carry

        lax.fori_loop(1, ff // UP_COLS, up_step, 0)
        act(ff // UP_COLS - 1)

        @pl.when(first)
        def _():
            w_copy(block, 5).wait()

        def down(lo, cols):
            part = dot_nn(gbuf[...], wd[:, lo:lo + cols]).astype(BF16)
            for f in range(fr):
                h = xs[v, f, :, lo:lo + cols].astype(F32) + part[f * npat:(f + 1) * npat].astype(F32)
                xs[v, f, :, lo:lo + cols] = h.astype(BF16)

        for lo in range(0, width, 512):
            down(lo, min(512, width - lo))

    def send_copy(v, peer, stage):
        if stage == 1:
            return pltpu.make_async_remote_copy(
                src_ref=ns.at[v, :, pl.ds(pl.multiple_of(peer * pp, pp), pp), :],
                dst_ref=rx.at[v, pl.ds(me * fr, fr)],
                send_sem=send1.at[v, peer], recv_sem=recv1.at[v, me],
                device_id={'sp': peer}, device_id_type=pl.DeviceIdType.MESH)
        return pltpu.make_async_remote_copy(
            src_ref=osend.at[v, pl.ds(peer * fr, fr)],
            dst_ref=orecv.at[v, :, pl.ds(pl.multiple_of(me * pp, pp), pp), :],
            send_sem=send2.at[v, peer], recv_sem=recv2.at[v, me],
            device_id={'sp': peer}, device_id_type=pl.DeviceIdType.MESH)

    def recv_wait(v, peer, stage):
        if stage == 1:
            dst = rx.at[v, pl.ds(peer * fr, fr)]
            sem = recv1.at[v, peer]
        else:
            dst = orecv.at[v, :, pl.ds(pl.multiple_of(peer * pp, pp), pp), :]
            sem = recv2.at[v, peer]
        pltpu.make_async_copy(dst, dst, sem).wait()

    def each_peer(fn):
        for step in range(1, n):
            fn(lax.rem(me + step, n))

    def spatial(v, carry):
        x_copy(v).wait()
        norm(v, 0, 0, to_nbuf)

        @pl.when(v == 0)
        def _():
            for which in range(3):
                w_copy(0, which).wait()

        for lo, hi in ((0, QKV_SPLIT), (QKV_SPLIT, 3 * width)):
            qkv[:, lo:hi] = dot_nt(nbuf[...], wq[lo:hi, :]).astype(BF16)

        @pl.when(v == nv - 1)
        def _():
            for which in range(3):
                w_copy(1, which).start()

        def store(f, t, val):
            obuf[f * npat:(f + 1) * npat, t * 128:(t + 1) * 128] = val.astype(BF16)

        attend([(f * npat, npat, h, functools.partial(store, f)) for f in range(fr) for h in range(heads)], lambda s: s)
        tail(v, 0, obuf[...], v == 0)

        @pl.when(v == nv - 1)
        def _():
            for which in range(3, 6):
                w_copy(1, which).start()

        def to_ns(f, r, val):
            ns[v, f, r:r + LN_ROWS, :] = val

        norm(v, 1, 0, to_ns)

        @pl.when(v == 0)
        def _():
            pl.semaphore_wait(barrier, n - 1)

        rx[v, pl.ds(me * fr, fr)] = ns[v, :, pl.ds(pl.multiple_of(me * pp, pp), pp), :]
        each_peer(lambda peer: send_copy(v, peer, 1).start())
        return carry

    lax.fori_loop(0, nv, spatial, 0)

    half = 8
    groups = pp // half
    grows = frames * half

    def temporal(v, carry):
        each_peer(lambda peer: recv_wait(v, peer, 1))

        @pl.when(v == 0)
        def _():
            for which in range(3):
                w_copy(1, which).wait()

        for lo, hi in ((0, QKV_SPLIT), (QKV_SPLIT, 3 * width)):
            val = dot_nt(rx[v].reshape(rows, width), wq[lo:hi, :]).reshape(frames, groups, half, hi - lo)
            for g in range(groups):
                qkv[g * grows:(g + 1) * grows, lo:hi] = val[:, g].reshape(grows, hi - lo).astype(BF16)

        sub = lax.broadcasted_iota(jnp.int32, (1, half, grows), 1)
        key = lax.broadcasted_iota(jnp.int32, (1, half, grows), 2)
        same = sub == lax.rem(key, half)

        def keep(s):
            return jnp.where(same, s.reshape(frames, half, grows), -jnp.inf).reshape(grows, grows)

        def store(g, t, val):
            of32[:, g, :, t * 128:(t + 1) * 128] = val.reshape(frames, half, 128)

        attend([(g * grows, grows, h, functools.partial(store, g)) for g in range(groups) for h in range(heads)], keep)
        for f in range(frames):
            osend[v, f] = of32[f].reshape(pp, width).astype(BF16)
        orecv[v, :, pl.ds(pl.multiple_of(me * pp, pp), pp), :] = osend[v, pl.ds(me * fr, fr)]
        each_peer(lambda peer: send_copy(v, peer, 2).start())
        return carry

    lax.fori_loop(0, nv, temporal, 0)

    def y_copy(v):
        return pltpu.make_async_copy(xs.at[v], y_hbm.at[v], ysem.at[v])

    def finish(v, carry):
        each_peer(lambda peer: recv_wait(v, peer, 2))
        tail(v, 1, orecv[v].reshape(rows, width), v == 0)
        y_copy(v).start()
        return carry

    lax.fori_loop(0, nv, finish, 0)
    for v in range(nv):
        y_copy(v).wait()
        each_peer(lambda peer: send_copy(v, peer, 1).wait_send())
        each_peer(lambda peer: send_copy(v, peer, 2).wait_send())


def solution(mesh):
    tok_spec = P(('pod', 'dp'), 'sp', None, None)
    n = mesh.shape['sp']

    def local_step(x, gain, shift, w_qkv, w_out, w_up, w_down):
        nv, fr, npat, width = x.shape
        heads, hd = w_qkv.shape[3:]
        ff = w_up.shape[2]
        rows = fr * npat
        wqkv_t = jnp.transpose(w_qkv, (0, 1, 3, 4, 2)).reshape(2, 3, heads * hd, width)
        wout_r = w_out.reshape(2, heads * hd, width)
        dims = (nv, fr, npat, width, heads, hd, ff, n)
        hbm = pl.BlockSpec(memory_space=pl.ANY)
        vmem = pl.BlockSpec(memory_space=pltpu.VMEM)
        pp, frames = npat // n, fr * n
        return pl.pallas_call(
            functools.partial(kernel, dims),
            out_shape=jax.ShapeDtypeStruct(x.shape, BF16),
            in_specs=[hbm, vmem, vmem, hbm, hbm, hbm, hbm],
            out_specs=hbm,
            scratch_shapes=[
                pltpu.VMEM((nv, fr, npat, width), BF16),
                pltpu.VMEM((nv, fr, npat, width), BF16),
                pltpu.VMEM((nv, frames, pp, width), BF16),
                pltpu.VMEM((nv, frames, pp, width), BF16),
                pltpu.VMEM((nv, fr, npat, width), BF16),
                pltpu.VMEM((3 * heads * hd, width), BF16),
                pltpu.VMEM((heads * hd, width), BF16),
                pltpu.VMEM((width, ff), BF16),
                pltpu.VMEM((ff, width), BF16),
                pltpu.VMEM((rows, width), BF16),
                pltpu.VMEM((rows, 3 * heads * hd), BF16),
                pltpu.VMEM((rows, heads * hd), BF16),
                pltpu.VMEM((rows, UP_COLS), BF16),
                pltpu.VMEM((rows, ff), BF16),
                pltpu.VMEM((frames, pp // 8, 8, width), F32),
                pltpu.VMEM((ATT_BUFS, frames * 8, frames * 8), F32),
                pltpu.VMEM((ATT_BUFS, frames * 8, frames * 8), BF16),
                pltpu.SemaphoreType.DMA((nv,)),
                pltpu.SemaphoreType.DMA((6,)),
                pltpu.SemaphoreType.DMA((nv,)),
                pltpu.SemaphoreType.DMA((nv, n)),
                pltpu.SemaphoreType.DMA((nv, n)),
                pltpu.SemaphoreType.DMA((nv, n)),
                pltpu.SemaphoreType.DMA((nv, n)),
            ],
            compiler_params=pltpu.CompilerParams(
                collective_id=0, has_side_effects=True, vmem_limit_bytes=67_000_000),
        )(x, gain, shift, wqkv_t, wout_r, w_up, w_down)

    return jax.shard_map(local_step, mesh=mesh, in_specs=(tok_spec, P(), P(), P(), P(), P(), P()), out_specs=tok_spec, check_vma=False)
```

```python
import functools

import jax
import jax.numpy as jnp
from jax import lax
from jax.experimental import pallas as pl
from jax.experimental.pallas import tpu as pltpu
from jax.sharding import PartitionSpec as P

LN_EPS = 1e-6
F32, BF16 = jnp.float32, jnp.bfloat16
UP_COLS = 512
DOWN_COLS = 512
LN_ROWS = 32
ATT_BUFS = 6
TILES_A = 5
TANH_IN = 0.7978845608028654
TANH_CUBE = 0.044715


def gelu(u):
    inner = u * (TANH_IN + (TANH_IN * TANH_CUBE) * (u * u))
    half = 0.5 * u
    return half + half * jnp.tanh(inner)


def dot_nt(a, b):
    return lax.dot_general(a, b, (((1,), (1,)), ((), ())), preferred_element_type=F32)


def dot_tn(a, b):
    return lax.dot_general(a, b, (((0,), (0,)), ((), ())), preferred_element_type=F32)


def dot_nn(a, b):
    return jnp.dot(a, b, preferred_element_type=F32)


def ln_rows(tok, gain, shift):
    mean = jnp.mean(tok, axis=-1, keepdims=True)
    cen = tok - mean
    var = jnp.mean(cen * cen, axis=-1, keepdims=True)
    return (cen * lax.rsqrt(var + LN_EPS) * gain + shift).astype(BF16)


def kernel(dims, x_hbm, gain_ref, shift_ref, wqkv_hbm, wout_hbm, wup_hbm, wdown_hbm, y_hbm,
           xs, ns, rx, osend, orecv, wq, wo, wu, wd, nbuf, qkv, obuf, ubuf, gbuf, of32, sbuf, pbuf, hbuf,
           xsem, wsem, qsem, ysem, send1, recv1, send2, recv2):
    nv, fr, npat, width, heads, hd, ff, n = dims
    rows = fr * npat
    pp = npat // n
    frames = fr * n
    me = lax.axis_index('sp')
    scale = hd ** -0.5
    barrier = pltpu.get_barrier_semaphore()

    def w_copy(block, which):
        src, dst = [(wout_hbm, wo), (wup_hbm, wu), (wdown_hbm, wd)][which - 3]
        return pltpu.make_async_copy(src.at[block], dst, wsem.at[which])

    def x_copy(v):
        return pltpu.make_async_copy(x_hbm.at[v], xs.at[v], xsem.at[v])

    x_copy(0).start()

    for step in range(1, n):
        peer = lax.rem(me + step, n)
        pl.semaphore_signal(barrier, inc=1, device_id={'sp': peer}, device_id_type=pl.DeviceIdType.MESH)

    tiles = width // 128
    cols_a, cols_b = TILES_A * 128, width - TILES_A * 128
    all_a = 3 * cols_a
    piece = 2 * 128

    def col(which, t):
        if t < TILES_A:
            return which * cols_a + t * 128
        return all_a + which * cols_b + (t - TILES_A) * 128

    def wq_copies(block):
        for which in range(3):
            for part in range(2):
                first, size = (0, cols_a) if part == 0 else (cols_a, cols_b)
                dst = col(which, 0 if part == 0 else TILES_A)
                yield pltpu.make_async_copy(wqkv_hbm.at[block, which, first:first + size],
                                            wq.at[dst:dst + size], qsem.at[which, part])

    def norm(read, block, which, write, lo=0, hi=rows):
        gain = gain_ref[block, which:which + 1, :].astype(F32)
        shift = shift_ref[block, which:which + 1, :].astype(F32)
        for r in range(lo, hi, LN_ROWS):
            write(r, ln_rows(read(r).astype(F32), gain, shift))

    def read_xs(v):
        return lambda r: xs[v, r:r + LN_ROWS, :]

    def to_nbuf(r, val):
        nbuf[r:r + LN_ROWS, :] = val

    def pass_on(v):
        def to_ns(r, val):
            ns[v, r // npat, r % npat:r % npat + LN_ROWS, :] = val

        norm(read_xs(v), 1, 0, to_ns)

    def send_on(v):
        rx[v, pl.ds(me * fr, fr)] = ns[v, :, pl.ds(pl.multiple_of(me * pp, pp), pp), :]
        each_peer(lambda peer: send_copy(v, peer, 1).start())

    def attend(units, group, keep, fill):
        lane = lax.broadcasted_iota(jnp.int32, (1, 128), 1)
        outs = {}
        tops, sums = {}, {}

        def span(h):
            return h * hd, (h + 1) * hd, h * hd // 128, ((h + 1) * hd - 1) // 128 + 1

        def cols(base, nrow, which, t0, t1):
            lo, hi = col(which, t0), col(which, t1 - 1) + 128
            if hi - lo == (t1 - t0) * 128:
                return qkv[base:base + nrow, lo:hi]
            return jnp.concatenate([qkv[base:base + nrow, col(which, t):col(which, t) + 128] for t in range(t0, t1)], axis=1)

        def buf(i):
            return i % ATT_BUFS

        def score(i):
            base, nrow, h = units[i][:3]
            lo, hi, t0, t1 = span(h)
            parts = []
            for t in range(t0, t1):
                part = cols(base, nrow, 1, t, t + 1)
                inside = (lane + t * 128 >= lo) & (lane + t * 128 < hi)
                parts.append(jnp.where(inside, part, jnp.zeros_like(part)))
            kw = parts[0] if len(parts) == 1 else jnp.concatenate(parts, axis=1)
            asks = cols(base, nrow, 0, t0, t1)
            sbuf[buf(i), :nrow, :nrow] = dot_nt(kw, asks)

        def scores(i):
            nrow = units[i][1]
            return sbuf[buf(i), :nrow, :nrow].reshape(nrow // group, group, nrow)

        def top(i):
            tops[i] = jnp.max(scores(i), axis=0, keepdims=True)
            if keep is None:
                tops[i] = jnp.max(tops[i], axis=1, keepdims=True)

        def expo(i):
            nrow = units[i][1]
            e = jnp.exp((scores(i) - tops.pop(i)) * scale)
            sbuf[buf(i), :nrow, :nrow] = e.reshape(nrow, nrow)
            total = jnp.sum(e, axis=0, keepdims=True)
            if keep is None:
                total = jnp.sum(total, axis=1, keepdims=True)
            inv = 1.0 / total
            sums[i] = inv if keep is None else jnp.where(keep, inv, 0.0)

        def prob(i):
            nrow = units[i][1]
            pbuf[buf(i), :nrow, :nrow] = (scores(i) * sums.pop(i)).reshape(nrow, nrow).astype(BF16)

        def mix(i):
            base, nrow, h, write = units[i]
            lo, hi, t0, t1 = span(h)
            o = dot_tn(pbuf[buf(i), :nrow, :nrow], cols(base, nrow, 2, t0, t1))
            for t in range(t0, t1):
                part = o[:, (t - t0) * 128:(t - t0 + 1) * 128]
                if (base, t) in outs:
                    part = jnp.where(lane + t * 128 >= lo, part, outs.pop((base, t)))
                if (t + 1) * 128 <= hi:
                    write(t, part)
                else:
                    outs[(base, t)] = part

        stages = ((score, 0), (top, 2), (expo, 3), (prob, 4), (mix, 5))
        early = sum(1 for unit in units if span(unit[2])[3] <= TILES_A)
        places = [k * early // len(fill) for k in range(len(fill))]
        for i in range(len(units) + 5):
            for k, place in enumerate(places):
                if i == place:
                    fill[k]()
            for fn, lag in reversed(stages):
                if 0 <= i - lag < len(units):
                    fn(i - lag)

    def tail(v, stage):
        first = v == 0

        @pl.when(first)
        def _():
            for which in range(3, 6):
                w_copy(stage, which).wait()

        step = rows // 2

        def out(lo):
            a = dot_nn(obuf[lo:lo + step, :], wo[...]).astype(BF16)
            hbuf[lo:lo + step, :] = (xs[v, lo:lo + step, :].astype(F32) + a.astype(F32)).astype(BF16)

        def up(c, lo, size):
            ubuf[c % 2, lo:lo + size] = dot_nn(nbuf[lo:lo + size, :], wu[:, c * UP_COLS:(c + 1) * UP_COLS]).astype(BF16)

        def mid(lo):
            norm(lambda r: hbuf[r:r + LN_ROWS, :], stage, 1, to_nbuf, lo, lo + step)

        chunks = ff // UP_COLS

        def act(c):
            gbuf[:, c * UP_COLS:(c + 1) * UP_COLS] = gelu(ubuf[c % 2].astype(F32)).astype(BF16)

        out(0)
        mid(0)
        out(step)
        up(0, 0, step)
        mid(step)
        up(0, step, step)
        for c in range(1, chunks):
            act(c - 1)
            up(c, 0, rows)
        act(chunks - 1)
        norm(read_xs(jnp.minimum(v + 1, nv - 1)), 0, 0, to_nbuf)
        for lo in range(0, width, DOWN_COLS):
            hi = min(width, lo + DOWN_COLS)
            part = dot_nn(gbuf[...], wd[:, lo:hi]).astype(BF16)
            xs[v, :, lo:hi] = (hbuf[:, lo:hi].astype(F32) + part.astype(F32)).astype(BF16)

    def send_copy(v, peer, stage):
        if stage == 1:
            return pltpu.make_async_remote_copy(
                src_ref=ns.at[v, :, pl.ds(pl.multiple_of(peer * pp, pp), pp), :],
                dst_ref=rx.at[v, pl.ds(me * fr, fr)],
                send_sem=send1.at[v, peer], recv_sem=recv1.at[v, me],
                device_id={'sp': peer}, device_id_type=pl.DeviceIdType.MESH)
        return pltpu.make_async_remote_copy(
            src_ref=osend.at[v, pl.ds(peer * fr, fr)],
            dst_ref=orecv.at[v, :, pl.ds(pl.multiple_of(me * pp, pp), pp), :],
            send_sem=send2.at[v, peer], recv_sem=recv2.at[v, me],
            device_id={'sp': peer}, device_id_type=pl.DeviceIdType.MESH)

    def recv_wait(v, peer, stage):
        if stage == 1:
            dst = rx.at[v, pl.ds(peer * fr, fr)]
            sem = recv1.at[v, peer]
        else:
            dst = orecv.at[v, :, pl.ds(pl.multiple_of(peer * pp, pp), pp), :]
            sem = recv2.at[v, peer]
        pltpu.make_async_copy(dst, dst, sem).wait()

    def each_peer(fn):
        for step in range(1, n):
            fn(lax.rem(me + step, n))

    def spatial(v):
        @pl.when(v == 0)
        def _():
            for copy in wq_copies(0):
                copy.wait()
            for which in range(3, 6):
                w_copy(0, which).start()
            x_copy(1).start()

        prev = jnp.maximum(v - 1, 0)
        qkv[:, :all_a] = dot_nt(nbuf[...], wq[:all_a, :]).astype(BF16)
        pass_on(prev)

        @pl.when(v == 0)
        def _():
            pl.semaphore_wait(barrier, n - 1)

        @pl.when(v > 0)
        def _():
            send_on(prev)

        @pl.when(v < nv - 1)
        def _():
            x_copy(v + 1).wait()

        @pl.when(v < nv - 2)
        def _():
            x_copy(v + 2).start()

        def store(f, t, val):
            obuf[f * npat:(f + 1) * npat, t * 128:(t + 1) * 128] = val.astype(BF16)

        def project(lo):
            qkv[:, lo:lo + piece] = dot_nt(nbuf[...], wq[lo:lo + piece, :]).astype(BF16)

        early = [h for h in range(heads) if (h + 1) * hd <= cols_a]
        order = [(f, h) for f in range(fr) for h in early] + [(f, h) for f in range(fr) for h in range(len(early), heads)]
        attend([(f * npat, npat, h, functools.partial(store, f)) for f, h in order], 8, None,
               [functools.partial(project, lo) for lo in range(all_a, 3 * width, piece)])

        @pl.when(v == nv - 1)
        def _():
            for copy in wq_copies(1):
                copy.start()

    half = 8
    groups = pp // half
    grows = frames * half

    def temporal(v, carry):
        each_peer(lambda peer: recv_wait(v, peer, 1))

        @pl.when(v == 0)
        def _():
            for copy in wq_copies(1):
                copy.wait()

        def project(lo, hi):
            val = dot_nt(rx[v].reshape(rows, width), wq[lo:hi, :]).reshape(frames, groups, half, hi - lo)
            for g in range(groups):
                qkv[g * grows:(g + 1) * grows, lo:hi] = val[:, g].reshape(grows, hi - lo).astype(BF16)

        project(0, all_a)
        sub = lax.broadcasted_iota(jnp.int32, (1, half, grows), 1)
        key = lax.broadcasted_iota(jnp.int32, (1, half, grows), 2)
        same = sub == lax.rem(key, half)

        def store(g, t, val):
            of32[:, g, :, t * 128:(t + 1) * 128] = val.reshape(frames, half, 128)

        early = [h for h in range(heads) if (h + 1) * hd <= cols_a]
        order = [(g, h) for g in range(groups) for h in early] + [(g, h) for g in range(groups) for h in range(len(early), heads)]
        attend([(g * grows, grows, h, functools.partial(store, g)) for g, h in order], half, same,
               [functools.partial(project, lo, lo + piece) for lo in range(all_a, 3 * width, piece)])
        for f in range(frames):
            osend[v, f] = of32[f].reshape(pp, width).astype(BF16)
        orecv[v, :, pl.ds(pl.multiple_of(me * pp, pp), pp), :] = osend[v, pl.ds(me * fr, fr)]
        each_peer(lambda peer: send_copy(v, peer, 2).start())
        return carry

    def y_copy(v):
        return pltpu.make_async_copy(xs.at[v], y_hbm.at[v], ysem.at[v])

    for copy in wq_copies(0):
        copy.start()
    x_copy(0).wait()
    norm(read_xs(0), 0, 0, to_nbuf)

    def phase(i, carry):
        stage = jnp.where(i >= nv, 1, 0)
        v = i - stage * nv

        @pl.when(i < nv)
        def _():
            spatial(v)

        @pl.when(i == nv)
        def _():
            pass_on(nv - 1)
            send_on(nv - 1)
            lax.fori_loop(0, nv, temporal, 0)

        @pl.when(i >= nv)
        def _():
            each_peer(lambda peer: recv_wait(v, peer, 2))
            obuf[...] = orecv[v].reshape(rows, width)

        tail(v, stage)

        @pl.when(i == nv - 1)
        def _():
            for which in range(3, 6):
                w_copy(1, which).start()

        @pl.when(i >= nv)
        def _():
            y_copy(v).start()

        return carry

    lax.fori_loop(0, 2 * nv, phase, 0)
    for v in range(nv):
        y_copy(v).wait()
        each_peer(lambda peer: send_copy(v, peer, 1).wait_send())
        each_peer(lambda peer: send_copy(v, peer, 2).wait_send())


def solution(mesh):
    tok_spec = P(('pod', 'dp'), 'sp', None, None)
    n = mesh.shape['sp']

    def local_step(x, gain, shift, w_qkv, w_out, w_up, w_down):
        nv, fr, npat, width = x.shape
        heads, hd = w_qkv.shape[3:]
        ff = w_up.shape[2]
        rows = fr * npat
        wqkv_t = jnp.transpose(w_qkv, (0, 1, 3, 4, 2)).reshape(2, 3, heads * hd, width)
        wout_r = w_out.reshape(2, heads * hd, width)
        dims = (nv, fr, npat, width, heads, hd, ff, n)
        hbm = pl.BlockSpec(memory_space=pl.ANY)
        vmem = pl.BlockSpec(memory_space=pltpu.VMEM)
        pp, frames = npat // n, fr * n
        y = pl.pallas_call(
            functools.partial(kernel, dims),
            out_shape=jax.ShapeDtypeStruct((nv, rows, width), BF16),
            in_specs=[hbm, vmem, vmem, hbm, hbm, hbm, hbm],
            out_specs=hbm,
            scratch_shapes=[
                pltpu.VMEM((nv, rows, width), BF16),
                pltpu.VMEM((nv, fr, npat, width), BF16),
                pltpu.VMEM((nv, frames, pp, width), BF16),
                pltpu.VMEM((nv, frames, pp, width), BF16),
                pltpu.VMEM((nv, fr, npat, width), BF16),
                pltpu.VMEM((3 * heads * hd, width), BF16),
                pltpu.VMEM((heads * hd, width), BF16),
                pltpu.VMEM((width, ff), BF16),
                pltpu.VMEM((ff, width), BF16),
                pltpu.VMEM((rows, width), BF16),
                pltpu.VMEM((rows, 3 * heads * hd), BF16),
                pltpu.VMEM((rows, heads * hd), BF16),
                pltpu.VMEM((2, rows, UP_COLS), BF16),
                pltpu.VMEM((rows, ff), BF16),
                pltpu.VMEM((frames, pp // 8, 8, width), F32),
                pltpu.VMEM((ATT_BUFS, frames * 8, frames * 8), F32),
                pltpu.VMEM((ATT_BUFS, frames * 8, frames * 8), BF16),
                pltpu.VMEM((rows, width), BF16),
                pltpu.SemaphoreType.DMA((nv,)),
                pltpu.SemaphoreType.DMA((6,)),
                pltpu.SemaphoreType.DMA((3, 2)),
                pltpu.SemaphoreType.DMA((nv,)),
                pltpu.SemaphoreType.DMA((nv, n)),
                pltpu.SemaphoreType.DMA((nv, n)),
                pltpu.SemaphoreType.DMA((nv, n)),
                pltpu.SemaphoreType.DMA((nv, n)),
            ],
            compiler_params=pltpu.CompilerParams(
                collective_id=0, has_side_effects=True, vmem_limit_bytes=67_000_000),
        )(x.reshape(nv, rows, width), gain, shift, wqkv_t, wout_r, w_up, w_down)
        return y.reshape(x.shape)

    return jax.shard_map(local_step, mesh=mesh, in_specs=(tok_spec, P(), P(), P(), P(), P(), P()), out_specs=tok_spec, check_vma=False)
```
